32 devices in a mesh: blk: 16 (over z, y, core), rel: 2 (over x).
Axes of the slice: x: 2, y: 2, z: 4, core: 2. Of those that a mesh axis runs over, the one named last changes fastest.
Arguments:
- source_table: float32 [400, 24576], P(None, ('blk', 'rel')), may hold values from -1.2 to 1.2
- source_state: float32 [24576], P(('blk', 'rel')), may hold values from 0.001 to 0.1
- target_table: float32 [400, 24576], P(None, ('blk', 'rel')), may hold values from -1.2 to 1.2
- target_state: float32 [24576], P(('blk', 'rel')), may hold values from 0.001 to 0.1
- relation_ops: float32 [400, 2048], P(None, 'blk'), may hold values from 0.5 to 1.5
- relation_state: float32 [400, 2048], P(None, 'blk'), may hold values from 0.01 to 1
- source_ids: int32 [2, 16384], P(None, ('blk', 'rel')), may hold values from 0 to 767
- target_ids: int32 [2, 16384], P(None, ('blk', 'rel')), may hold values from 0 to 767
- relation_ids: int32 [2, 16384], P(None, ('blk', 'rel')), may hold values from 0 to 127
- negative_ids: int32 [2, 16384], P(None, ('blk', 'rel')), may hold values from 0 to 767
Outputs:
- new_source: float32 [400, 24576], P(None, ('blk', 'rel'))
- new_source_state: float32 [24576], P(('blk', 'rel'))
- held_target: float32 [400, 24576], P(None, ('blk', 'rel'))
- held_target_state: float32 [24576], P(('blk', 'rel'))
- new_relations: float32 [400, 2048], P(None, 'blk')
- new_relation_state: float32 [400, 2048], P(None, 'blk')
The draws below stay inside these ranges and needn't reach their ends.
All inputs are finite; a program needn't handle non-finite values.
Results may differ from the reference program's by a relative error of at most 0.0001.
Values sent between devices are 32-bit elements; how exact they have to be, the bound alone decides.
A program may use at most 64 MiB of HBM per device.

```python
import math
import jax
import jax.numpy as jnp
from jax import lax

D = 400
ROWS = 768
EDGE_DEV = 512
NEG_DEV = 512
REL_DEV = 128
BUCKETS = 2
ENTITIES = 24576
EDGES = 16384
NEGS = 16384
RELS = 2048
N_BLK = 16
N_REL = 2


def touch_ends(entries, own_key, low, top_value):
    spot = [jax.random.randint(jax.random.fold_in(own_key, axis), (), 0, length) for axis, length in enumerate(entries.shape)]
    main_axis = entries.shape.index(max(entries.shape))
    beside = spot[:main_axis] + [(spot[main_axis] + 1) % entries.shape[main_axis]] + spot[main_axis + 1:]
    return entries.at[tuple(spot)].set(low).at[tuple(beside)].set(top_value)


def shard_levels(rng, shape, split, smallest, high):
    def one(dim, blocks):
        heights = jax.random.uniform(jax.random.fold_in(jax.random.fold_in(rng, 6), dim), (blocks,), jnp.float32, smallest / len(split), high / len(split))
        return jnp.repeat(jnp.exp(heights), shape[dim] // blocks).reshape((-1,) + (1,) * (len(shape) - dim - 1))

    gain = one(*split[0])
    for cut in split[1:]:
        gain = gain * one(*cut)
    return gain


def bell_draw(rng, shape, deviation, limit, shards=(), dtype=jnp.bfloat16):
    gain = shard_levels(rng, shape, shards, -0.22, 0.18) if shards else 1.0
    drawn = jax.random.normal(rng, shape, jnp.float32) * deviation * gain
    return jnp.minimum(jnp.maximum(drawn, -limit), limit).astype(dtype)


def setup_inputs(seed: int = 0) -> dict:
    streams_of = jax.random.split(jax.random.key(seed), 11)
    source_table = bell_draw(streams_of[0], (D, ENTITIES), 0.2, 1.2, ((1, 32),), jnp.float32)
    source_state = jnp.clip(jnp.exp(math.log(0.1) - 4.6051702 * jax.random.uniform(streams_of[1], (ENTITIES,), jnp.float32) ** shard_levels(streams_of[1], (ENTITIES,), ((0, 32),), -0.2, 0.2)), 0.001, 0.1)
    target_table = bell_draw(streams_of[2], (D, ENTITIES), 0.2, 1.2, ((1, 32),), jnp.float32)
    target_state = jnp.clip(jnp.exp(math.log(0.1) - 4.6051702 * jax.random.uniform(streams_of[3], (ENTITIES,), jnp.float32) ** shard_levels(streams_of[3], (ENTITIES,), ((0, 32),), -0.2, 0.2)), 0.001, 0.1)
    relation_ops = jnp.clip(0.5 + 1.0 * jax.random.uniform(streams_of[4], (D, RELS), jnp.float32) ** shard_levels(streams_of[4], (D, RELS), ((1, 16),), -0.2, 0.2), 0.5, 1.5)
    relation_state = jnp.clip(jnp.exp(math.log(1.0) - 4.6051702 * jax.random.uniform(streams_of[5], (D, RELS), jnp.float32) ** shard_levels(streams_of[5], (D, RELS), ((1, 16),), -0.2, 0.2)), 0.01, 1.0)
    source_ids = touch_ends(jax.random.randint(streams_of[6], (BUCKETS, EDGES), 0, ROWS), jax.random.fold_in(streams_of[6], 1), 0, ROWS - 1).astype(jnp.int32)
    target_ids = touch_ends(jax.random.randint(streams_of[7], (BUCKETS, EDGES), 0, ROWS), jax.random.fold_in(streams_of[7], 1), 0, ROWS - 1).astype(jnp.int32)
    relation_ids = touch_ends(jax.random.randint(streams_of[8], (BUCKETS, EDGES), 0, REL_DEV), jax.random.fold_in(streams_of[8], 1), 0, REL_DEV - 1).astype(jnp.int32)
    negative_ids = touch_ends(jax.random.randint(streams_of[9], (BUCKETS, NEGS), 0, ROWS), jax.random.fold_in(streams_of[9], 1), 0, ROWS - 1).astype(jnp.int32)
    return {"source_table": source_table, "source_state": source_state, "target_table": target_table, "target_state": target_state, "relation_ops": relation_ops, "relation_state": relation_state, "source_ids": source_ids, "target_ids": target_ids, "relation_ids": relation_ids, "negative_ids": negative_ids}


learn_rate = 0.1
epsilon = 1e-06
HIGHEST = lax.Precision.HIGHEST

def row_adagrad(matrix, row_state, gradient):
    fresh = row_state + lax.optimization_barrier(jnp.mean(gradient * gradient, axis=0))
    return (matrix - learn_rate * gradient / (jnp.sqrt(fresh) + epsilon)[None, :], fresh)

def slice_step(source_side, source_rows, target_side, target_rows, relations, source_idx, target_idx, relation_idx, negative_idx):
    source = jnp.take(source_side, source_idx, axis=1)
    target = jnp.take(target_side, target_idx, axis=1)
    negative = jnp.take(target_side, negative_idx, axis=1)
    relation = jnp.take(relations, relation_idx, axis=1)
    queries = source * relation
    positive = lax.optimization_barrier(jnp.sum(queries * target, axis=0))
    neg_score = lax.dot_general(queries, negative, (((0,), (0,)), ((), ())), precision=HIGHEST)
    pos_coef = -jax.nn.sigmoid(-positive)
    neg_coef = jax.nn.sigmoid(neg_score) / negative_idx.shape[0]
    grad_query = target * pos_coef[None, :] + lax.dot_general(negative, neg_coef, (((1,), (1,)), ((), ())), precision=HIGHEST)
    grad_target = queries * pos_coef[None, :]
    grad_negative = jnp.dot(queries, neg_coef, precision=HIGHEST)
    target_grad = jnp.zeros_like(target_side).at[:, target_idx].add(grad_target).at[:, negative_idx].add(grad_negative)
    source_grad = jnp.zeros_like(source_side).at[:, source_idx].add(grad_query * relation)
    relation_grad = jnp.zeros_like(relations).at[:, relation_idx].add(grad_query * source)
    new_target, new_target_rows = row_adagrad(target_side, target_rows, target_grad)
    new_source, new_source_rows = row_adagrad(source_side, source_rows, source_grad)
    return (new_source, new_source_rows, new_target, new_target_rows, relation_grad)

def reference(source_table, source_state, target_table, target_state, relation_ops, relation_state, source_ids, target_ids, relation_ids, negative_ids):
    slice_count = N_BLK * N_REL

    def split_table(matrix):
        return matrix.reshape(D, slice_count, ROWS).transpose(1, 0, 2)

    def join_table(blocks):
        return blocks.transpose(1, 0, 2).reshape(D, slice_count * ROWS)
    source_blocks = split_table(source_table)
    source_rows = source_state.reshape(slice_count, ROWS)
    target_blocks = split_table(target_table)
    target_rows = target_state.reshape(slice_count, ROWS)
    relation_blocks = relation_ops.reshape(D, N_BLK, REL_DEV).transpose(1, 0, 2)
    source_split = source_ids.reshape(BUCKETS, slice_count, EDGE_DEV)
    target_split = target_ids.reshape(BUCKETS, slice_count, EDGE_DEV)
    relation_split = relation_ids.reshape(BUCKETS, slice_count, EDGE_DEV)
    negative_split = negative_ids.reshape(BUCKETS, slice_count, NEG_DEV)
    owners = (jnp.arange(slice_count) // N_REL).astype(jnp.int32)
    summed = jnp.zeros((N_BLK, D, REL_DEV), jnp.float32)

    def per_slice(items):
        src_side, src_rows, tgt_side, tgt_rows, owner, src_idx, tgt_idx, rel_idx, neg_idx = items
        return slice_step(src_side, src_rows, tgt_side, tgt_rows, relation_blocks[owner], src_idx, tgt_idx, rel_idx, neg_idx)
    for bucket in range(BUCKETS):
        if bucket > 0:
            target_blocks = jnp.roll(target_blocks, N_REL, axis=0)
            target_rows = jnp.roll(target_rows, N_REL, axis=0)
        source_blocks, source_rows, target_blocks, target_rows, relation_grads = lax.map(per_slice, (source_blocks, source_rows, target_blocks, target_rows, owners, source_split[bucket], target_split[bucket], relation_split[bucket], negative_split[bucket]))
        summed = summed + relation_grads.reshape(N_BLK, N_REL, D, REL_DEV).sum(axis=1)
    summed_flat = summed.transpose(1, 0, 2).reshape(D, N_BLK * REL_DEV)
    new_relation_state = relation_state + summed_flat * summed_flat
    new_relations = relation_ops - learn_rate * summed_flat / (jnp.sqrt(new_relation_state) + epsilon)
    return (join_table(source_blocks), source_rows.reshape(slice_count * ROWS), join_table(target_blocks), target_rows.reshape(slice_count * ROWS), new_relations, new_relation_state)
```

```python
import functools

import jax
import jax.numpy as jnp
from jax import lax
from jax.experimental import pallas as pl
from jax.experimental.pallas import tpu as pltpu
from jax.sharding import PartitionSpec as P

learn_rate = 0.1
epsilon = 1e-06
MESH = pl.DeviceIdType.MESH
F32 = jnp.float32
BF16 = jnp.bfloat16


def split(x):
    high = x.astype(BF16)
    return high, (x - high.astype(F32)).astype(BF16)


def nn(a, b):
    return lax.dot_general(a, b, (((1,), (0,)), ((), ())), preferred_element_type=F32)


def nt(a, b):
    return lax.dot_general(a, b, (((1,), (1,)), ((), ())), preferred_element_type=F32)


def kernel(
    n_blk, n_rel, chunk,
    src_ref, srow_ref, tgt_ref, trow_ref, rel_ref, rstate_ref, sid_ref, rid_ref, tid_ref, nid_ref,
    out_src, out_srow, out_tgt, out_trow, out_rel, out_rstate,
    hot, rhot, table3, weight_hi, weight_lo, q3t, q_hi, q_lo, picked, relation, counts,
    send, recv, rel_all, send_sem, recv_sem, rsend_sem, rrecv_sem,
):
    dims, rows = src_ref.shape
    buckets, edges = sid_ref.shape
    negs = nid_ref.shape[1]
    rels = rel_ref.shape[1]
    chunks = rows // chunk
    pad = send.shape[2] - dims
    my_blk = lax.axis_index("blk")
    my_rel = lax.axis_index("rel")
    nxt = lax.rem(my_blk + 1, n_blk)
    prv = lax.rem(my_blk + n_blk - 1, n_blk)

    barrier = pltpu.get_barrier_semaphore()
    for other in (nxt, prv):
        pl.semaphore_signal(barrier, inc=1, device_id={"blk": other}, device_id_type=MESH)
    for step in range(1, n_rel):
        pl.semaphore_signal(
            barrier, inc=1, device_id={"rel": lax.rem(my_rel + step, n_rel)}, device_id_type=MESH
        )
    pl.semaphore_wait(barrier, 2 + n_rel - 1)

    def hop(bucket, c):
        return pltpu.make_async_remote_copy(
            src_ref=send.at[bucket, c],
            dst_ref=recv.at[bucket, c],
            send_sem=send_sem.at[bucket, c],
            recv_sem=recv_sem.at[bucket, c],
            device_id={"blk": nxt},
            device_id_type=MESH,
        )

    for bucket in range(buckets):
        last = bucket + 1 == buckets
        now_src = src_ref if bucket == 0 else out_src
        now_srow = srow_ref if bucket == 0 else out_srow
        sid = sid_ref[pl.ds(bucket, 1), :]
        rid = rid_ref[pl.ds(bucket, 1), :]
        hot[...] = (lax.broadcasted_iota(jnp.int32, (rows, edges), 0) == sid).astype(F32).astype(BF16)
        rhot[...] = (lax.broadcasted_iota(jnp.int32, (rels, edges), 0) == rid).astype(F32).astype(BF16)
        s_hi, s_lo = split(now_src[...])
        picked[...] = nn(s_hi, hot[...]) + nn(s_lo, hot[...])
        r_hi, r_lo = split(rel_ref[...])
        relation[...] = nn(r_hi, rhot[...]) + nn(r_lo, rhot[...])
        queries = picked[...] * relation[...]
        hi, lo = split(queries)
        q_hi[...] = hi
        q_lo[...] = lo
        hi_t = jnp.transpose(hi.astype(F32)).astype(BF16)
        lo_t = jnp.transpose(lo.astype(F32)).astype(BF16)
        q3t[0] = hi_t
        q3t[1] = lo_t
        tid = tid_ref[bucket]
        nid = nid_ref[bucket]

        for c in range(chunks):
            cols = pl.ds(c * chunk, chunk)
            lane = lax.broadcasted_iota(jnp.int32, (negs, chunk), 1) + c * chunk
            counts[:, cols] = jnp.sum(
                (lane == nid).astype(F32), axis=0, keepdims=True
            ) * (1.0 / negs)

        def do_chunk(c, carry):
            if bucket == 0:
                cols = pl.ds(pl.multiple_of(c * chunk, chunk), chunk)
                table = tgt_ref[:, cols]
                state = trow_ref[:, cols]
            else:
                cols = pl.ds(pl.multiple_of(c * chunk, chunk), chunk)
                hop(bucket - 1, c).wait_recv()
                table = recv[bucket - 1, c, :dims, :]
                state = recv[bucket - 1, c, dims:dims + 1, :]
            t_hi, t_lo = split(table)
            table3[0, c] = t_hi
            table3[1, c] = t_lo
            score = nn(q3t[0], t_hi) + nn(q3t[0], t_lo) + nn(q3t[1], t_hi)
            small = jnp.exp(-jnp.abs(score))
            large = 1.0 / (1.0 + small)
            small = small * large
            up = score >= 0
            sig = jnp.where(up, large, small)
            co = jnp.where(up, small, large)
            lane = lax.broadcasted_iota(jnp.int32, (edges, chunk), 1) + c * chunk
            weight = counts[:, cols] * sig - jnp.where(lane == tid, co, 0.0)
            w_hi, w_lo = split(weight)
            weight_hi[c] = w_hi
            weight_lo[c] = w_lo
            grad = nn(q_hi[...], w_hi) + nn(q_hi[...], w_lo) + nn(q_lo[...], w_hi)
            fresh = state + jnp.sum(grad * grad, axis=0, keepdims=True) * (1.0 / dims)
            new = table - grad * (learn_rate / (jnp.sqrt(fresh) + epsilon))
            if last:
                out_tgt[:, cols] = new
                out_trow[:, cols] = fresh
            else:
                send[bucket, c, :dims, :] = new
                send[bucket, c, dims:, :] = jnp.broadcast_to(fresh, (pad, chunk))
                hop(bucket, c).start()
            return carry

        lax.fori_loop(0, chunks, do_chunk, 0)

        grad_query = jnp.zeros((dims, edges), F32)
        for c in range(chunks):
            grad_query += (
                nt(table3[0, c], weight_hi[c])
                + nt(table3[0, c], weight_lo[c])
                + nt(table3[1, c], weight_hi[c])
            )
        g_hi, g_lo = split(grad_query * picked[...])
        rel_grad = nt(g_hi, rhot[...]) + nt(g_lo, rhot[...])
        if bucket == 0:
            rel_all[my_rel] = rel_grad
        else:
            rel_all[my_rel] = rel_all[my_rel] + rel_grad
        if last:
            for step in range(1, n_rel):
                peer = lax.rem(my_rel + step, n_rel)
                pltpu.make_async_remote_copy(
                    src_ref=rel_all.at[my_rel],
                    dst_ref=rel_all.at[my_rel],
                    send_sem=rsend_sem.at[step - 1],
                    recv_sem=rrecv_sem.at[my_rel],
                    device_id={"rel": peer},
                    device_id_type=MESH,
                ).start()
        g_hi, g_lo = split(grad_query * relation[...])
        src_grad = nt(g_hi, hot[...]) + nt(g_lo, hot[...])
        fresh = now_srow[...] + jnp.sum(src_grad * src_grad, axis=0, keepdims=True) * (1.0 / dims)
        out_src[...] = now_src[...] - src_grad * (learn_rate / (jnp.sqrt(fresh) + epsilon))
        out_srow[...] = fresh

    for bucket in range(buckets - 1):
        for c in range(chunks):
            hop(bucket, c).wait_send()
    for step in range(1, n_rel):
        peer = lax.rem(my_rel + n_rel - step, n_rel)
        arrived = pltpu.make_async_remote_copy(
            src_ref=rel_all.at[peer],
            dst_ref=rel_all.at[peer],
            send_sem=rsend_sem.at[step - 1],
            recv_sem=rrecv_sem.at[peer],
            device_id={"rel": peer},
            device_id_type=MESH,
        )
        arrived.wait_send()
        arrived.wait_recv()
    total = rel_all[0]
    for step in range(1, n_rel):
        total = total + rel_all[step]
    new_state = rstate_ref[...] + total * total
    out_rstate[...] = new_state
    out_rel[...] = rel_ref[...] - learn_rate * total / (jnp.sqrt(new_state) + epsilon)


def solution(mesh):
    n_blk, n_rel = mesh.shape["blk"], mesh.shape["rel"]

    def per_device(
        source_table, source_state, target_table, target_state, relation_ops, relation_state,
        source_ids, target_ids, relation_ids, negative_ids,
    ):
        dims, rows = source_table.shape
        rels = relation_ops.shape[1]
        buckets, edges = source_ids.shape
        chunk = 256 if rows % 256 == 0 else 128
        chunks = rows // chunk
        vmem = pl.BlockSpec(memory_space=pltpu.VMEM)
        shape = jax.ShapeDtypeStruct
        out = pl.pallas_call(
            functools.partial(kernel, n_blk, n_rel, chunk),
            out_shape=(
                shape((dims, rows), F32), shape((1, rows), F32),
                shape((dims, rows), F32), shape((1, rows), F32),
                shape((dims, rels), F32), shape((dims, rels), F32),
            ),
            in_specs=[vmem] * 10,
            out_specs=(vmem,) * 6,
            scratch_shapes=[
                pltpu.VMEM((rows, edges), BF16),
                pltpu.VMEM((rels, edges), BF16),
                pltpu.VMEM((2, chunks, dims, chunk), BF16),
                pltpu.VMEM((chunks, edges, chunk), BF16),
                pltpu.VMEM((chunks, edges, chunk), BF16),
                pltpu.VMEM((2, edges, dims), BF16),
                pltpu.VMEM((dims, edges), BF16),
                pltpu.VMEM((dims, edges), BF16),
                pltpu.VMEM((dims, edges), F32),
                pltpu.VMEM((dims, edges), F32),
                pltpu.VMEM((1, rows), F32),
                pltpu.VMEM((buckets - 1, chunks, dims + 8, chunk), F32),
                pltpu.VMEM((buckets - 1, chunks, dims + 8, chunk), F32),
                pltpu.VMEM((n_rel, dims, rels), F32),
                pltpu.SemaphoreType.DMA((buckets - 1, chunks)),
                pltpu.SemaphoreType.DMA((buckets - 1, chunks)),
                pltpu.SemaphoreType.DMA((n_rel,)),
                pltpu.SemaphoreType.DMA((n_rel,)),
            ],
            compiler_params=pltpu.CompilerParams(
                collective_id=0, has_side_effects=True, vmem_limit_bytes=60 * 1024 * 1024
            ),
        )(
            source_table, source_state[None, :], target_table, target_state[None, :],
            relation_ops, relation_state, source_ids, relation_ids,
            target_ids[:, :, None], negative_ids[:, :, None],
        )
        return (out[0], out[1][0], out[2], out[3][0], out[4], out[5])

    split_both = ("blk", "rel")
    return jax.shard_map(
        per_device,
        mesh=mesh,
        in_specs=(
            P(None, split_both), P(split_both), P(None, split_both), P(split_both),
            P(None, "blk"), P(None, "blk"),
            P(None, split_both), P(None, split_both), P(None, split_both), P(None, split_both),
        ),
        out_specs=(
            P(None, split_both), P(split_both), P(None, split_both), P(split_both),
            P(None, "blk"), P(None, "blk"),
        ),
        check_vma=False,
    )
```

```python
import functools

import jax
import jax.numpy as jnp
from jax import lax
from jax.experimental import pallas as pl
from jax.experimental.pallas import tpu as pltpu
from jax.sharding import PartitionSpec as P

learn_rate = 0.1
epsilon = 1e-06
MESH = pl.DeviceIdType.MESH
F32 = jnp.float32
BF16 = jnp.bfloat16


def split(x):
    high = x.astype(BF16)
    return high, (x - high.astype(F32)).astype(BF16)


def nn(a, b):
    return lax.dot_general(a, b, (((1,), (0,)), ((), ())), preferred_element_type=F32)


def nt(a, b):
    return lax.dot_general(a, b, (((1,), (1,)), ((), ())), preferred_element_type=F32)


def column(row):
    wide = jnp.broadcast_to(row.astype(F32), (8, row.shape[1]))
    return jnp.transpose(wide)[:, :1].astype(jnp.int32)


def emit(*refs):
    half = len(refs) // 2
    inputs, outputs, sem = refs[:half], refs[half:-1], refs[-1]
    copies = []
    for i in (0, 2, 4, 5):
        copies.append(pltpu.make_async_copy(inputs[i], outputs[i], sem.at[i]))
        copies[-1].start()
    for i in (1, 3):
        outputs[i][...] = inputs[i][0, :]
    for copy in copies:
        copy.wait()


def kernel(
    n_blk, n_rel, chunk,
    src_in, srow_in, tgt_in, trow_in, rel_in, rstate_in, sid_in, rid_in, tid_in, nid_in,
    out_src, out_srow, out_tgt, out_trow, out_rel, out_rstate,
    src_ref, srow_ref, tgt_ref, trow_ref, rel_ref, rstate_ref, sid_ref, rid_ref, tid_ref, nid_ref,
    load_sem, hot, rhot, table3, weight_hi, weight_lo, q3t, q_hi, q_lo, picked, relation, gq_ref, counts,
    send, recv, rel_all, send_sem, recv_sem, rsend_sem, rrecv_sem,
):
    loads = {}
    for index, (there, here) in enumerate((
        (sid_in, sid_ref), (rid_in, rid_ref), (rel_in, rel_ref), (src_in, src_ref), (tid_in, tid_ref),
        (nid_in, nid_ref), (trow_in, trow_ref), (tgt_in, tgt_ref), (srow_in, srow_ref), (rstate_in, rstate_ref),
    )):
        loads[index] = pltpu.make_async_copy(there, here, load_sem.at[index])
        loads[index].start()
    dims, rows = src_ref.shape
    buckets, edges = sid_ref.shape
    negs = nid_ref.shape[1]
    rels = rel_ref.shape[1]
    chunks = rows // chunk
    pad = send.shape[2] - dims
    my_blk = lax.axis_index("blk")
    my_rel = lax.axis_index("rel")
    nxt = lax.rem(my_blk + 1, n_blk)
    prv = lax.rem(my_blk + n_blk - 1, n_blk)

    barrier = pltpu.get_barrier_semaphore()
    for other in (nxt, prv):
        pl.semaphore_signal(barrier, inc=1, device_id={"blk": other}, device_id_type=MESH)
    for step in range(1, n_rel):
        pl.semaphore_signal(
            barrier, inc=1, device_id={"rel": lax.rem(my_rel + step, n_rel)}, device_id_type=MESH
        )

    def hop(bucket, c):
        return pltpu.make_async_remote_copy(
            src_ref=send.at[bucket, c],
            dst_ref=recv.at[bucket, c],
            send_sem=send_sem.at[bucket, c],
            recv_sem=recv_sem.at[bucket, c],
            device_id={"blk": nxt},
            device_id_type=MESH,
        )

    for index in range(4):
        loads[index].wait()

    for bucket in range(buckets):
        last = bucket + 1 == buckets
        now_src = src_ref if bucket == 0 else out_src
        sid = sid_ref[pl.ds(bucket, 1), :]
        rid = rid_ref[pl.ds(bucket, 1), :]
        hot[...] = (lax.broadcasted_iota(jnp.int32, (rows, edges), 0) == sid).astype(F32).astype(BF16)
        rhot[...] = (lax.broadcasted_iota(jnp.int32, (rels, edges), 0) == rid).astype(F32).astype(BF16)
        s_hi, s_lo = split(now_src[...])
        picked[...] = nn(s_hi, hot[...]) + nn(s_lo, hot[...])
        r_hi, r_lo = split(rel_ref[...])
        relation[...] = nn(r_hi, rhot[...]) + nn(r_lo, rhot[...])
        queries = picked[...] * relation[...]
        hi, lo = split(queries)
        q_hi[...] = hi
        q_lo[...] = lo
        hi_t = jnp.transpose(hi.astype(F32)).astype(BF16)
        lo_t = jnp.transpose(lo.astype(F32)).astype(BF16)
        q3t[0] = hi_t
        q3t[1] = lo_t
        if bucket == 0:
            for index in range(4, 10):
                loads[index].wait()
        tid = column(tid_ref[pl.ds(bucket, 1), :])
        nid = column(nid_ref[pl.ds(bucket, 1), :])

        for c in range(chunks):
            cols = pl.ds(c * chunk, chunk)
            lane = lax.broadcasted_iota(jnp.int32, (negs, chunk), 1) + c * chunk
            counts[:, cols] = jnp.sum(
                (lane == nid).astype(F32), axis=0, keepdims=True
            ) * (1.0 / negs)

        if bucket == 0:
            pl.semaphore_wait(barrier, 2 + n_rel - 1)

        def do_chunk(c, carry):
            if bucket == 0:
                cols = pl.ds(pl.multiple_of(c * chunk, chunk), chunk)
                table = tgt_ref[:, cols]
                state = trow_ref[cols].reshape(1, chunk)
            else:
                cols = pl.ds(pl.multiple_of(c * chunk, chunk), chunk)
                hop(bucket - 1, c).wait_recv()
                table = recv[bucket - 1, c, :dims, :]
                state = recv[bucket - 1, c, dims:dims + 1, :]
            t_hi, t_lo = split(table)
            if bucket == 0:
                table3[0, c] = t_hi
                table3[1, c] = t_lo
            score = nn(q3t[0], t_hi) + nn(q3t[0], t_lo) + nn(q3t[1], t_hi)
            small = jnp.exp(-jnp.abs(score))
            large = 1.0 / (1.0 + small)
            small = small * large
            up = score >= 0
            sig = jnp.where(up, large, small)
            co = jnp.where(up, small, large)
            lane = lax.broadcasted_iota(jnp.int32, (edges, chunk), 1) + c * chunk
            weight = counts[:, cols] * sig - jnp.where(lane == tid, co, 0.0)
            w_hi, w_lo = split(weight)
            if bucket == 0:
                weight_hi[c] = w_hi
                weight_lo[c] = w_lo
            else:
                gq_ref[...] += nt(t_hi, w_hi) + nt(t_hi, w_lo) + nt(t_lo, w_hi)
            grad = nn(q_hi[...], w_hi) + nn(q_hi[...], w_lo) + nn(q_lo[...], w_hi)
            fresh = state + jnp.sum(grad * grad, axis=0, keepdims=True) * (1.0 / dims)
            new = table - grad * (learn_rate / (jnp.sqrt(fresh) + epsilon))
            if last:
                out_tgt[:, cols] = new
                out_trow[:, cols] = fresh
            else:
                send[bucket, c, :dims, :] = new
                send[bucket, c, dims:, :] = jnp.broadcast_to(fresh, (pad, chunk))
                hop(bucket, c).start()
            return carry

        if bucket > 0:
            gq_ref[...] = jnp.zeros_like(gq_ref)
        lax.fori_loop(0, chunks, do_chunk, 0)

        if bucket == 0:
            grad_query = jnp.zeros((dims, edges), F32)
            for c in range(chunks):
                grad_query += (
                    nt(table3[0, c], weight_hi[c])
                    + nt(table3[0, c], weight_lo[c])
                    + nt(table3[1, c], weight_hi[c])
                )
        else:
            grad_query = gq_ref[...]
        g_hi, g_lo = split(grad_query * picked[...])
        rel_grad = nt(g_hi, rhot[...]) + nt(g_lo, rhot[...])
        if bucket == 0:
            rel_all[my_rel] = rel_grad
        else:
            rel_all[my_rel] = rel_all[my_rel] + rel_grad
        if last:
            for step in range(1, n_rel):
                peer = lax.rem(my_rel + step, n_rel)
                pltpu.make_async_remote_copy(
                    src_ref=rel_all.at[my_rel],
                    dst_ref=rel_all.at[my_rel],
                    send_sem=rsend_sem.at[step - 1],
                    recv_sem=rrecv_sem.at[my_rel],
                    device_id={"rel": peer},
                    device_id_type=MESH,
                ).start()
        g_hi, g_lo = split(grad_query * relation[...])
        src_grad = nt(g_hi, hot[...]) + nt(g_lo, hot[...])
        now_srow = srow_ref[...].reshape(1, rows) if bucket == 0 else out_srow[...]
        fresh = now_srow + jnp.sum(src_grad * src_grad, axis=0, keepdims=True) * (1.0 / dims)
        out_src[...] = now_src[...] - src_grad * (learn_rate / (jnp.sqrt(fresh) + epsilon))
        out_srow[...] = fresh

    for bucket in range(buckets - 1):
        for c in range(chunks):
            hop(bucket, c).wait_send()
    for step in range(1, n_rel):
        peer = lax.rem(my_rel + n_rel - step, n_rel)
        arrived = pltpu.make_async_remote_copy(
            src_ref=rel_all.at[peer],
            dst_ref=rel_all.at[peer],
            send_sem=rsend_sem.at[step - 1],
            recv_sem=rrecv_sem.at[peer],
            device_id={"rel": peer},
            device_id_type=MESH,
        )
        arrived.wait_send()
        arrived.wait_recv()
    total = rel_all[0]
    for step in range(1, n_rel):
        total = total + rel_all[step]
    new_state = rstate_ref[...] + total * total
    out_rstate[...] = new_state
    out_rel[...] = rel_ref[...] - learn_rate * total / (jnp.sqrt(new_state) + epsilon)


def solution(mesh):
    n_blk, n_rel = mesh.shape["blk"], mesh.shape["rel"]

    def per_device(
        source_table, source_state, target_table, target_state, relation_ops, relation_state,
        source_ids, target_ids, relation_ids, negative_ids,
    ):
        dims, rows = source_table.shape
        rels = relation_ops.shape[1]
        buckets, edges = source_ids.shape
        chunk = 256 if rows % 256 == 0 else 128
        chunks = rows // chunk
        vmem = pl.BlockSpec(memory_space=pltpu.VMEM)
        shape = jax.ShapeDtypeStruct
        out = pl.pallas_call(
            functools.partial(kernel, n_blk, n_rel, chunk),
            out_shape=(
                pltpu.VMEM((dims, rows), F32), pltpu.VMEM((1, rows), F32),
                pltpu.VMEM((dims, rows), F32), pltpu.VMEM((1, rows), F32),
                pltpu.VMEM((dims, rels), F32), pltpu.VMEM((dims, rels), F32),
            ),
            in_specs=[pl.BlockSpec(memory_space=pltpu.HBM)] * 10,
            out_specs=(vmem,) * 6,
            scratch_shapes=[
                pltpu.VMEM((dims, rows), F32), pltpu.VMEM((rows,), F32),
                pltpu.VMEM((dims, rows), F32), pltpu.VMEM((rows,), F32),
                pltpu.VMEM((dims, rels), F32), pltpu.VMEM((dims, rels), F32),
                *[pltpu.VMEM(ids.shape, jnp.int32) for ids in (source_ids, relation_ids, target_ids, negative_ids)],
                pltpu.SemaphoreType.DMA((10,)),
                pltpu.VMEM((rows, edges), BF16),
                pltpu.VMEM((rels, edges), BF16),
                pltpu.VMEM((2, chunks, dims, chunk), BF16),
                pltpu.VMEM((chunks, edges, chunk), BF16),
                pltpu.VMEM((chunks, edges, chunk), BF16),
                pltpu.VMEM((2, edges, dims), BF16),
                pltpu.VMEM((dims, edges), BF16),
                pltpu.VMEM((dims, edges), BF16),
                pltpu.VMEM((dims, edges), F32),
                pltpu.VMEM((dims, edges), F32),
                pltpu.VMEM((dims, edges), F32),
                pltpu.VMEM((1, rows), F32),
                pltpu.VMEM((buckets - 1, chunks, dims + 8, chunk), F32),
                pltpu.VMEM((buckets - 1, chunks, dims + 8, chunk), F32),
                pltpu.VMEM((n_rel, dims, rels), F32),
                pltpu.SemaphoreType.DMA((buckets - 1, chunks)),
                pltpu.SemaphoreType.DMA((buckets - 1, chunks)),
                pltpu.SemaphoreType.DMA((n_rel,)),
                pltpu.SemaphoreType.DMA((n_rel,)),
            ],
            compiler_params=pltpu.CompilerParams(
                collective_id=0, has_side_effects=True, vmem_limit_bytes=40 * 1024 * 1024
            ),
        )(*(
            pltpu.with_memory_space_constraint(x, pltpu.HBM) for x in (
                source_table, source_state, target_table, target_state,
                relation_ops, relation_state, source_ids, relation_ids,
                target_ids, negative_ids,
            )
        ))
        hbm = pl.BlockSpec(memory_space=pl.ANY)
        return pl.pallas_call(
            emit,
            out_shape=(
                shape((dims, rows), F32), shape((rows,), F32),
                shape((dims, rows), F32), shape((rows,), F32),
                shape((dims, rels), F32), shape((dims, rels), F32),
            ),
            in_specs=[vmem] * 6,
            out_specs=(hbm, vmem, hbm, vmem, hbm, hbm),
            scratch_shapes=[pltpu.SemaphoreType.DMA((6,))],
            compiler_params=pltpu.CompilerParams(vmem_limit_bytes=16 * 1024 * 1024),
        )(*out)

    split_both = ("blk", "rel")
    return jax.shard_map(
        per_device,
        mesh=mesh,
        in_specs=(
            P(None, split_both), P(split_both), P(None, split_both), P(split_both),
            P(None, "blk"), P(None, "blk"),
            P(None, split_both), P(None, split_both), P(None, split_both), P(None, split_both),
        ),
        out_specs=(
            P(None, split_both), P(split_both), P(None, split_both), P(split_both),
            P(None, "blk"), P(None, "blk"),
        ),
        check_vma=False,
    )
```

```python
import functools

import jax
import jax.numpy as jnp
from jax import lax
from jax.experimental import pallas as pl
from jax.experimental.pallas import tpu as pltpu
from jax.sharding import PartitionSpec as P

learn_rate = 0.1
epsilon = 1e-06
MESH = pl.DeviceIdType.MESH
F32 = jnp.float32
BF16 = jnp.bfloat16


def split(x):
    high = x.astype(BF16)
    return high, (x - high.astype(F32)).astype(BF16)


def nn(a, b):
    return lax.dot_general(a, b, (((1,), (0,)), ((), ())), preferred_element_type=F32)


def nt(a, b):
    return lax.dot_general(a, b, (((1,), (1,)), ((), ())), preferred_element_type=F32)


def column(row):
    wide = jnp.broadcast_to(row.astype(F32), (8, row.shape[1]))
    return jnp.transpose(wide)[:, :1].astype(jnp.int32)


def emit(*refs):
    inputs, outputs, (first, second, sem) = refs[:6], refs[6:12], refs[12:]
    copies = []
    for i in (0, 2, 4, 5):
        copies.append(pltpu.make_async_copy(inputs[i], outputs[i], sem.at[i]))
        copies[-1].start()
    for i, line in ((1, first), (3, second)):
        line[...] = inputs[i][0, :]
        copies.append(pltpu.make_async_copy(line, outputs[i], sem.at[i]))
        copies[-1].start()
    for copy in copies:
        copy.wait()


def kernel(
    n_blk, n_rel, chunk,
    src_in, srow_in, tgt_in, trow_in, rel_in, rstate_in, sid_in, rid_in, tid_in, nid_in,
    out_src, out_srow, out_tgt, out_trow, out_rel, out_rstate,
    src_ref, srow_ref, tgt_ref, trow_ref, rel_ref, rstate_ref, sid_ref, rid_ref, tid_ref, nid_ref,
    load_sem, hot, rhot, table3, weight_hi, weight_lo, q3t, q_hi, q_lo, picked, relation, gq_ref, counts,
    send, recv, rel_all, send_sem, recv_sem, rsend_sem, rrecv_sem,
):
    loads = {}
    for index, (there, here) in enumerate((
        (sid_in, sid_ref), (rid_in, rid_ref), (rel_in, rel_ref), (src_in, src_ref), (tid_in, tid_ref),
        (nid_in, nid_ref), (trow_in, trow_ref), (tgt_in, tgt_ref), (srow_in, srow_ref), (rstate_in, rstate_ref),
    )):
        loads[index] = pltpu.make_async_copy(there, here, load_sem.at[index])
        loads[index].start()
    dims, rows = src_ref.shape
    buckets, edges = sid_ref.shape
    negs = nid_ref.shape[1]
    rels = rel_ref.shape[1]
    chunks = rows // chunk
    pad = send.shape[2] - dims
    my_blk = lax.axis_index("blk")
    my_rel = lax.axis_index("rel")
    nxt = lax.rem(my_blk + 1, n_blk)
    prv = lax.rem(my_blk + n_blk - 1, n_blk)

    barrier = pltpu.get_barrier_semaphore()
    for other in (nxt, prv):
        pl.semaphore_signal(barrier, inc=1, device_id={"blk": other}, device_id_type=MESH)
    for step in range(1, n_rel):
        pl.semaphore_signal(
            barrier, inc=1, device_id={"rel": lax.rem(my_rel + step, n_rel)}, device_id_type=MESH
        )

    def hop(bucket, c):
        return pltpu.make_async_remote_copy(
            src_ref=send.at[bucket, c],
            dst_ref=recv.at[bucket, c],
            send_sem=send_sem.at[bucket, c],
            recv_sem=recv_sem.at[bucket, c],
            device_id={"blk": nxt},
            device_id_type=MESH,
        )

    for index in range(4):
        loads[index].wait()

    for bucket in range(buckets):
        last = bucket + 1 == buckets
        now_src = src_ref if bucket == 0 else out_src
        sid = sid_ref[pl.ds(bucket, 1), :]
        rid = rid_ref[pl.ds(bucket, 1), :]
        hot[...] = (lax.broadcasted_iota(jnp.int32, (rows, edges), 0) == sid).astype(F32).astype(BF16)
        rhot[...] = (lax.broadcasted_iota(jnp.int32, (rels, edges), 0) == rid).astype(F32).astype(BF16)
        s_hi, s_lo = split(now_src[...])
        picked[...] = nn(s_hi, hot[...]) + nn(s_lo, hot[...])
        r_hi, r_lo = split(rel_ref[...])
        relation[...] = nn(r_hi, rhot[...]) + nn(r_lo, rhot[...])
        queries = picked[...] * relation[...]
        hi, lo = split(queries)
        q_hi[...] = hi
        q_lo[...] = lo
        hi_t = jnp.transpose(hi.astype(F32)).astype(BF16)
        lo_t = jnp.transpose(lo.astype(F32)).astype(BF16)
        q3t[0] = hi_t
        q3t[1] = lo_t
        if bucket == 0:
            for index in range(4, 10):
                loads[index].wait()
        tid = column(tid_ref[pl.ds(bucket, 1), :])
        nid = column(nid_ref[pl.ds(bucket, 1), :])

        for c in range(chunks):
            cols = pl.ds(c * chunk, chunk)
            lane = lax.broadcasted_iota(jnp.int32, (negs, chunk), 1) + c * chunk
            counts[:, cols] = jnp.sum(
                (lane == nid).astype(F32), axis=0, keepdims=True
            ) * (1.0 / negs)

        if bucket == 0:
            pl.semaphore_wait(barrier, 2 + n_rel - 1)

        def weigh(c):
            cols = pl.ds(pl.multiple_of(c * chunk, chunk), chunk)
            if bucket == 0:
                table = tgt_ref[:, cols]
            else:
                hop(bucket - 1, c).wait_recv()
                table = recv[bucket - 1, c, :dims, :]
            t_hi, t_lo = split(table)
            if bucket == 0:
                table3[0, c] = t_hi
                table3[1, c] = t_lo
            score = nn(q3t[0], t_hi) + nn(q3t[0], t_lo) + nn(q3t[1], t_hi)
            small = jnp.exp(-jnp.abs(score))
            large = 1.0 / (1.0 + small)
            small = small * large
            up = score >= 0
            sig = jnp.where(up, large, small)
            co = jnp.where(up, small, large)
            lane = lax.broadcasted_iota(jnp.int32, (edges, chunk), 1) + c * chunk
            weight = counts[:, cols] * sig - jnp.where(lane == tid, co, 0.0)
            w_hi, w_lo = split(weight)
            weight_hi[c] = w_hi
            weight_lo[c] = w_lo
            if bucket > 0:
                part = nt(t_hi, w_hi) + nt(t_hi, w_lo) + nt(t_lo, w_hi)
                gq_ref[...] = part if isinstance(c, int) and c == 0 else gq_ref[...] + part

        def finish(c):
            cols = pl.ds(pl.multiple_of(c * chunk, chunk), chunk)
            if bucket == 0:
                table = tgt_ref[:, cols]
                state = trow_ref[cols].reshape(1, chunk)
            else:
                table = recv[bucket - 1, c, :dims, :]
                state = recv[bucket - 1, c, dims:dims + 1, :]
            w_hi = weight_hi[c]
            w_lo = weight_lo[c]
            grad = nn(q_hi[...], w_hi) + nn(q_hi[...], w_lo) + nn(q_lo[...], w_hi)
            fresh = state + jnp.sum(grad * grad, axis=0, keepdims=True) * (1.0 / dims)
            new = table - grad * (learn_rate / (jnp.sqrt(fresh) + epsilon))
            if last:
                out_tgt[:, cols] = new
                out_trow[:, cols] = fresh
            else:
                send[bucket, c, :dims, :] = new
                send[bucket, c, dims:, :] = jnp.broadcast_to(fresh, (pad, chunk))
                hop(bucket, c).start()

        if bucket == 0:

            def both(c, carry):
                weigh(c)
                finish(c)
                return carry

            lax.fori_loop(0, chunks, both, 0)
        else:
            for c in range(chunks):
                weigh(c)
                if not last or c + 1 < chunks:
                    finish(c)
        if bucket == 0:
            grad_query = jnp.zeros((dims, edges), F32)
            for c in range(chunks):
                grad_query += (
                    nt(table3[0, c], weight_hi[c])
                    + nt(table3[0, c], weight_lo[c])
                    + nt(table3[1, c], weight_hi[c])
                )
        else:
            grad_query = gq_ref[...]
        g_hi, g_lo = split(grad_query * picked[...])
        rel_grad = nt(g_hi, rhot[...]) + nt(g_lo, rhot[...])
        if bucket == 0:
            rel_all[my_rel] = rel_grad
        else:
            rel_all[my_rel] = rel_all[my_rel] + rel_grad
        if last:
            for step in range(1, n_rel):
                peer = lax.rem(my_rel + step, n_rel)
                pltpu.make_async_remote_copy(
                    src_ref=rel_all.at[my_rel],
                    dst_ref=rel_all.at[my_rel],
                    send_sem=rsend_sem.at[step - 1],
                    recv_sem=rrecv_sem.at[my_rel],
                    device_id={"rel": peer},
                    device_id_type=MESH,
                ).start()
        if last and bucket > 0:
            finish(chunks - 1)
        g_hi, g_lo = split(grad_query * relation[...])
        src_grad = nt(g_hi, hot[...]) + nt(g_lo, hot[...])
        now_srow = srow_ref[...].reshape(1, rows) if bucket == 0 else out_srow[...]
        fresh = now_srow + jnp.sum(src_grad * src_grad, axis=0, keepdims=True) * (1.0 / dims)
        out_src[...] = now_src[...] - src_grad * (learn_rate / (jnp.sqrt(fresh) + epsilon))
        out_srow[...] = fresh

    for bucket in range(buckets - 1):
        for c in range(chunks):
            hop(bucket, c).wait_send()
    for step in range(1, n_rel):
        peer = lax.rem(my_rel + n_rel - step, n_rel)
        arrived = pltpu.make_async_remote_copy(
            src_ref=rel_all.at[peer],
            dst_ref=rel_all.at[peer],
            send_sem=rsend_sem.at[step - 1],
            recv_sem=rrecv_sem.at[peer],
            device_id={"rel": peer},
            device_id_type=MESH,
        )
        arrived.wait_send()
        arrived.wait_recv()
    total = rel_all[0]
    for step in range(1, n_rel):
        total = total + rel_all[step]
    new_state = rstate_ref[...] + total * total
    out_rstate[...] = new_state
    out_rel[...] = rel_ref[...] - learn_rate * total / (jnp.sqrt(new_state) + epsilon)


def solution(mesh):
    n_blk, n_rel = mesh.shape["blk"], mesh.shape["rel"]

    def per_device(
        source_table, source_state, target_table, target_state, relation_ops, relation_state,
        source_ids, target_ids, relation_ids, negative_ids,
    ):
        dims, rows = source_table.shape
        rels = relation_ops.shape[1]
        buckets, edges = source_ids.shape
        chunk = 256 if rows % 256 == 0 else 128
        chunks = rows // chunk
        vmem = pl.BlockSpec(memory_space=pltpu.VMEM)
        shape = jax.ShapeDtypeStruct
        out = pl.pallas_call(
            functools.partial(kernel, n_blk, n_rel, chunk),
            out_shape=(
                pltpu.VMEM((dims, rows), F32), pltpu.VMEM((1, rows), F32),
                pltpu.VMEM((dims, rows), F32), pltpu.VMEM((1, rows), F32),
                pltpu.VMEM((dims, rels), F32), pltpu.VMEM((dims, rels), F32),
            ),
            in_specs=[pl.BlockSpec(memory_space=pltpu.HBM)] * 10,
            out_specs=(vmem,) * 6,
            scratch_shapes=[
                pltpu.VMEM((dims, rows), F32), pltpu.VMEM((rows,), F32),
                pltpu.VMEM((dims, rows), F32), pltpu.VMEM((rows,), F32),
                pltpu.VMEM((dims, rels), F32), pltpu.VMEM((dims, rels), F32),
                *[pltpu.VMEM(ids.shape, jnp.int32) for ids in (source_ids, relation_ids, target_ids, negative_ids)],
                pltpu.SemaphoreType.DMA((10,)),
                pltpu.VMEM((rows, edges), BF16),
                pltpu.VMEM((rels, edges), BF16),
                pltpu.VMEM((2, chunks, dims, chunk), BF16),
                pltpu.VMEM((chunks, edges, chunk), BF16),
                pltpu.VMEM((chunks, edges, chunk), BF16),
                pltpu.VMEM((2, edges, dims), BF16),
                pltpu.VMEM((dims, edges), BF16),
                pltpu.VMEM((dims, edges), BF16),
                pltpu.VMEM((dims, edges), F32),
                pltpu.VMEM((dims, edges), F32),
                pltpu.VMEM((dims, edges), F32),
                pltpu.VMEM((1, rows), F32),
                pltpu.VMEM((buckets - 1, chunks, dims + 8, chunk), F32),
                pltpu.VMEM((buckets - 1, chunks, dims + 8, chunk), F32),
                pltpu.VMEM((n_rel, dims, rels), F32),
                pltpu.SemaphoreType.DMA((buckets - 1, chunks)),
                pltpu.SemaphoreType.DMA((buckets - 1, chunks)),
                pltpu.SemaphoreType.DMA((n_rel,)),
                pltpu.SemaphoreType.DMA((n_rel,)),
            ],
            compiler_params=pltpu.CompilerParams(
                collective_id=0, has_side_effects=True, vmem_limit_bytes=40 * 1024 * 1024
            ),
        )(*(
            pltpu.with_memory_space_constraint(x, pltpu.HBM) for x in (
                source_table, source_state, target_table, target_state,
                relation_ops, relation_state, source_ids, relation_ids,
                target_ids, negative_ids,
            )
        ))
        hbm = pl.BlockSpec(memory_space=pl.ANY)
        return pl.pallas_call(
            emit,
            out_shape=(
                shape((dims, rows), F32), shape((rows,), F32),
                shape((dims, rows), F32), shape((rows,), F32),
                shape((dims, rels), F32), shape((dims, rels), F32),
            ),
            in_specs=[vmem] * 6,
            out_specs=(hbm,) * 6,
            scratch_shapes=[pltpu.VMEM((rows,), F32), pltpu.VMEM((rows,), F32), pltpu.SemaphoreType.DMA((6,))],
            compiler_params=pltpu.CompilerParams(vmem_limit_bytes=16 * 1024 * 1024),
        )(*out)

    split_both = ("blk", "rel")
    return jax.shard_map(
        per_device,
        mesh=mesh,
        in_specs=(
            P(None, split_both), P(split_both), P(None, split_both), P(split_both),
            P(None, "blk"), P(None, "blk"),
            P(None, split_both), P(None, split_both), P(None, split_both), P(None, split_both),
        ),
        out_specs=(
            P(None, split_both), P(split_both), P(None, split_both), P(split_both),
            P(None, "blk"), P(None, "blk"),
        ),
        check_vma=False,
    )
```

```python
import functools

import jax
import jax.numpy as jnp
from jax import lax
from jax.experimental import pallas as pl
from jax.experimental.pallas import tpu as pltpu
from jax.sharding import PartitionSpec as P

learn_rate = 0.1
epsilon = 1e-06
MESH = pl.DeviceIdType.MESH
F32 = jnp.float32
BF16 = jnp.bfloat16


def split(x):
    high = x.astype(BF16)
    return high, (x - high.astype(F32)).astype(BF16)


def nn(a, b):
    return lax.dot_general(a, b, (((1,), (0,)), ((), ())), preferred_element_type=F32)


def nt(a, b):
    return lax.dot_general(a, b, (((1,), (1,)), ((), ())), preferred_element_type=F32)


def column(row):
    wide = jnp.broadcast_to(row.astype(F32), (8, row.shape[1]))
    return jnp.transpose(wide)[:, :1].astype(jnp.int32)


def emit(*refs):
    inputs, outputs, (first, second, sem) = refs[:6], refs[6:12], refs[12:]
    copies = []
    for i in (0, 2, 4, 5):
        copies.append(pltpu.make_async_copy(inputs[i], outputs[i], sem.at[i]))
        copies[-1].start()
    for i, line in ((1, first), (3, second)):
        line[...] = inputs[i][0, :]
        copies.append(pltpu.make_async_copy(line, outputs[i], sem.at[i]))
        copies[-1].start()
    for copy in copies:
        copy.wait()


def kernel(
    n_blk, n_rel, chunk,
    src_in, srow_in, tgt_in, trow_in, rel_in, rstate_in, sid_in, rid_in, tid_in, nid_in,
    out_src, out_srow, out_tgt, out_trow, out_rel, out_rstate,
    src_ref, srow_ref, tgt_ref, trow_ref, rel_ref, rstate_ref, sid_ref, rid_ref, tid_ref, nid_ref,
    load_sem, hot, rhot, table3, weight_hi, weight_lo, q3t, q_hi, q_lo, picked, relation, gq_ref, counts,
    send, recv, rel_all, send_sem, recv_sem, rsend_sem, rrecv_sem,
):
    loads = {}
    for index, (there, here) in enumerate((
        (sid_in, sid_ref), (rid_in, rid_ref), (tid_in, tid_ref), (nid_in, nid_ref), (rel_in, rel_ref),
        (src_in, src_ref), (trow_in, trow_ref), (tgt_in, tgt_ref), (srow_in, srow_ref), (rstate_in, rstate_ref),
    )):
        loads[index] = pltpu.make_async_copy(there, here, load_sem.at[index])
        loads[index].start()
    dims, rows = src_ref.shape
    buckets, edges = sid_ref.shape
    negs = nid_ref.shape[1]
    rels = rel_ref.shape[1]
    chunks = rows // chunk
    pad = send.shape[2] - dims
    my_blk = lax.axis_index("blk")
    my_rel = lax.axis_index("rel")
    nxt = lax.rem(my_blk + 1, n_blk)
    prv = lax.rem(my_blk + n_blk - 1, n_blk)

    barrier = pltpu.get_barrier_semaphore()
    for other in (nxt, prv):
        pl.semaphore_signal(barrier, inc=1, device_id={"blk": other}, device_id_type=MESH)
    for step in range(1, n_rel):
        pl.semaphore_signal(
            barrier, inc=1, device_id={"rel": lax.rem(my_rel + step, n_rel)}, device_id_type=MESH
        )

    def hop(bucket, c):
        return pltpu.make_async_remote_copy(
            src_ref=send.at[bucket, c],
            dst_ref=recv.at[bucket, c],
            send_sem=send_sem.at[bucket, c],
            recv_sem=recv_sem.at[bucket, c],
            device_id={"blk": nxt},
            device_id_type=MESH,
        )

    for index in range(4):
        loads[index].wait()

    for bucket in range(buckets):
        last = bucket + 1 == buckets
        now_src = src_ref if bucket == 0 else out_src
        sid = sid_ref[pl.ds(bucket, 1), :]
        rid = rid_ref[pl.ds(bucket, 1), :]
        hot[...] = (lax.broadcasted_iota(jnp.int32, (rows, edges), 0) == sid).astype(F32).astype(BF16)
        rhot[...] = (lax.broadcasted_iota(jnp.int32, (rels, edges), 0) == rid).astype(F32).astype(BF16)
        tid = column(tid_ref[pl.ds(bucket, 1), :])
        nid = column(nid_ref[pl.ds(bucket, 1), :])

        for c in range(chunks):
            cols = pl.ds(c * chunk, chunk)
            lane = lax.broadcasted_iota(jnp.int32, (negs, chunk), 1) + c * chunk
            counts[:, cols] = jnp.sum(
                (lane == nid).astype(F32), axis=0, keepdims=True
            ) * (1.0 / negs)

        if bucket == 0:
            for index in range(4, 6):
                loads[index].wait()
        s_hi, s_lo = split(now_src[...])
        picked[...] = nn(s_hi, hot[...]) + nn(s_lo, hot[...])
        r_hi, r_lo = split(rel_ref[...])
        relation[...] = nn(r_hi, rhot[...]) + nn(r_lo, rhot[...])
        queries = picked[...] * relation[...]
        hi, lo = split(queries)
        q_hi[...] = hi
        q_lo[...] = lo
        hi_t = jnp.transpose(hi.astype(F32)).astype(BF16)
        lo_t = jnp.transpose(lo.astype(F32)).astype(BF16)
        q3t[0] = hi_t
        q3t[1] = lo_t
        if bucket == 0:
            for index in range(6, 10):
                loads[index].wait()
        if bucket == 0:
            pl.semaphore_wait(barrier, 2 + n_rel - 1)

        def weigh(c):
            cols = pl.ds(pl.multiple_of(c * chunk, chunk), chunk)
            if bucket == 0:
                table = tgt_ref[:, cols]
            else:
                hop(bucket - 1, c).wait_recv()
                table = recv[bucket - 1, c, :dims, :]
            t_hi, t_lo = split(table)
            if bucket == 0:
                table3[0, c] = t_hi
                table3[1, c] = t_lo
            score = nn(q3t[0], t_hi) + nn(q3t[0], t_lo) + nn(q3t[1], t_hi)
            small = jnp.exp(-jnp.abs(score))
            large = 1.0 / (1.0 + small)
            small = small * large
            up = score >= 0
            sig = jnp.where(up, large, small)
            co = jnp.where(up, small, large)
            lane = lax.broadcasted_iota(jnp.int32, (edges, chunk), 1) + c * chunk
            weight = counts[:, cols] * sig - jnp.where(lane == tid, co, 0.0)
            w_hi, w_lo = split(weight)
            weight_hi[c] = w_hi
            weight_lo[c] = w_lo
            if bucket > 0:
                part = nt(t_hi, w_hi) + nt(t_hi, w_lo) + nt(t_lo, w_hi)
                gq_ref[...] = part if isinstance(c, int) and c == 0 else gq_ref[...] + part

        def finish(c):
            cols = pl.ds(pl.multiple_of(c * chunk, chunk), chunk)
            if bucket == 0:
                table = tgt_ref[:, cols]
                state = trow_ref[cols].reshape(1, chunk)
            else:
                table = recv[bucket - 1, c, :dims, :]
                state = recv[bucket - 1, c, dims:dims + 1, :]
            w_hi = weight_hi[c]
            w_lo = weight_lo[c]
            grad = nn(q_hi[...], w_hi) + nn(q_hi[...], w_lo) + nn(q_lo[...], w_hi)
            fresh = state + jnp.sum(grad * grad, axis=0, keepdims=True) * (1.0 / dims)
            new = table - grad * (learn_rate / (jnp.sqrt(fresh) + epsilon))
            if last:
                out_tgt[:, cols] = new
                out_trow[:, cols] = fresh
            else:
                send[bucket, c, :dims, :] = new
                send[bucket, c, dims:, :] = jnp.broadcast_to(fresh, (pad, chunk))
                hop(bucket, c).start()

        if bucket == 0:

            def both(c, carry):
                weigh(c)
                finish(c)
                return carry

            lax.fori_loop(0, chunks, both, 0)
        else:
            for c in range(chunks):
                weigh(c)
                if not last or c + 1 < chunks:
                    finish(c)
        if bucket == 0:
            grad_query = jnp.zeros((dims, edges), F32)
            for c in range(chunks):
                grad_query += (
                    nt(table3[0, c], weight_hi[c])
                    + nt(table3[0, c], weight_lo[c])
                    + nt(table3[1, c], weight_hi[c])
                )
        else:
            grad_query = gq_ref[...]
        g_hi, g_lo = split(grad_query * picked[...])
        rel_grad = nt(g_hi, rhot[...]) + nt(g_lo, rhot[...])
        if bucket == 0:
            rel_all[my_rel] = rel_grad
        else:
            rel_all[my_rel] = rel_all[my_rel] + rel_grad
        if last:
            for step in range(1, n_rel):
                peer = lax.rem(my_rel + step, n_rel)
                pltpu.make_async_remote_copy(
                    src_ref=rel_all.at[my_rel],
                    dst_ref=rel_all.at[my_rel],
                    send_sem=rsend_sem.at[step - 1],
                    recv_sem=rrecv_sem.at[my_rel],
                    device_id={"rel": peer},
                    device_id_type=MESH,
                ).start()
        if last and bucket > 0:
            finish(chunks - 1)
        g_hi, g_lo = split(grad_query * relation[...])
        src_grad = nt(g_hi, hot[...]) + nt(g_lo, hot[...])
        now_srow = srow_ref[...].reshape(1, rows) if bucket == 0 else out_srow[...]
        fresh = now_srow + jnp.sum(src_grad * src_grad, axis=0, keepdims=True) * (1.0 / dims)
        out_src[...] = now_src[...] - src_grad * (learn_rate / (jnp.sqrt(fresh) + epsilon))
        out_srow[...] = fresh

    for bucket in range(buckets - 1):
        for c in range(chunks):
            hop(bucket, c).wait_send()
    for step in range(1, n_rel):
        peer = lax.rem(my_rel + n_rel - step, n_rel)
        arrived = pltpu.make_async_remote_copy(
            src_ref=rel_all.at[peer],
            dst_ref=rel_all.at[peer],
            send_sem=rsend_sem.at[step - 1],
            recv_sem=rrecv_sem.at[peer],
            device_id={"rel": peer},
            device_id_type=MESH,
        )
        arrived.wait_send()
        arrived.wait_recv()
    total = rel_all[0]
    for step in range(1, n_rel):
        total = total + rel_all[step]
    new_state = rstate_ref[...] + total * total
    out_rstate[...] = new_state
    out_rel[...] = rel_ref[...] - learn_rate * total / (jnp.sqrt(new_state) + epsilon)


def solution(mesh):
    n_blk, n_rel = mesh.shape["blk"], mesh.shape["rel"]

    def per_device(
        source_table, source_state, target_table, target_state, relation_ops, relation_state,
        source_ids, target_ids, relation_ids, negative_ids,
    ):
        dims, rows = source_table.shape
        rels = relation_ops.shape[1]
        buckets, edges = source_ids.shape
        chunk = 256 if rows % 256 == 0 else 128
        chunks = rows // chunk
        vmem = pl.BlockSpec(memory_space=pltpu.VMEM)
        shape = jax.ShapeDtypeStruct
        out = pl.pallas_call(
            functools.partial(kernel, n_blk, n_rel, chunk),
            out_shape=(
                pltpu.VMEM((dims, rows), F32), pltpu.VMEM((1, rows), F32),
                pltpu.VMEM((dims, rows), F32), pltpu.VMEM((1, rows), F32),
                pltpu.VMEM((dims, rels), F32), pltpu.VMEM((dims, rels), F32),
            ),
            in_specs=[pl.BlockSpec(memory_space=pltpu.HBM)] * 10,
            out_specs=(vmem,) * 6,
            scratch_shapes=[
                pltpu.VMEM((dims, rows), F32), pltpu.VMEM((rows,), F32),
                pltpu.VMEM((dims, rows), F32), pltpu.VMEM((rows,), F32),
                pltpu.VMEM((dims, rels), F32), pltpu.VMEM((dims, rels), F32),
                *[pltpu.VMEM(ids.shape, jnp.int32) for ids in (source_ids, relation_ids, target_ids, negative_ids)],
                pltpu.SemaphoreType.DMA((10,)),
                pltpu.VMEM((rows, edges), BF16),
                pltpu.VMEM((rels, edges), BF16),
                pltpu.VMEM((2, chunks, dims, chunk), BF16),
                pltpu.VMEM((chunks, edges, chunk), BF16),
                pltpu.VMEM((chunks, edges, chunk), BF16),
                pltpu.VMEM((2, edges, dims), BF16),
                pltpu.VMEM((dims, edges), BF16),
                pltpu.VMEM((dims, edges), BF16),
                pltpu.VMEM((dims, edges), F32),
                pltpu.VMEM((dims, edges), F32),
                pltpu.VMEM((dims, edges), F32),
                pltpu.VMEM((1, rows), F32),
                pltpu.VMEM((buckets - 1, chunks, dims + 8, chunk), F32),
                pltpu.VMEM((buckets - 1, chunks, dims + 8, chunk), F32),
                pltpu.VMEM((n_rel, dims, rels), F32),
                pltpu.SemaphoreType.DMA((buckets - 1, chunks)),
                pltpu.SemaphoreType.DMA((buckets - 1, chunks)),
                pltpu.SemaphoreType.DMA((n_rel,)),
                pltpu.SemaphoreType.DMA((n_rel,)),
            ],
            compiler_params=pltpu.CompilerParams(
                collective_id=0, has_side_effects=True, vmem_limit_bytes=40 * 1024 * 1024
            ),
        )(*(
            pltpu.with_memory_space_constraint(x, pltpu.HBM) for x in (
                source_table, source_state, target_table, target_state,
                relation_ops, relation_state, source_ids, relation_ids,
                target_ids, negative_ids,
            )
        ))
        hbm = pl.BlockSpec(memory_space=pl.ANY)
        return pl.pallas_call(
            emit,
            out_shape=(
                shape((dims, rows), F32), shape((rows,), F32),
                shape((dims, rows), F32), shape((rows,), F32),
                shape((dims, rels), F32), shape((dims, rels), F32),
            ),
            in_specs=[vmem] * 6,
            out_specs=(hbm,) * 6,
            scratch_shapes=[pltpu.VMEM((rows,), F32), pltpu.VMEM((rows,), F32), pltpu.SemaphoreType.DMA((6,))],
            compiler_params=pltpu.CompilerParams(vmem_limit_bytes=16 * 1024 * 1024),
        )(*out)

    split_both = ("blk", "rel")
    return jax.shard_map(
        per_device,
        mesh=mesh,
        in_specs=(
            P(None, split_both), P(split_both), P(None, split_both), P(split_both),
            P(None, "blk"), P(None, "blk"),
            P(None, split_both), P(None, split_both), P(None, split_both), P(None, split_both),
        ),
        out_specs=(
            P(None, split_both), P(split_both), P(None, split_both), P(split_both),
            P(None, "blk"), P(None, "blk"),
        ),
        check_vma=False,
    )
```
